768 devices in a mesh: dp: 48 (over x_lo, z, core), tp: 16 (over x_hi, y).
Axes of the slice: x: 4 (x_hi: 2, x_lo: 2; x = x_hi * 2 + x_lo), y: 8, z: 12, core: 2. Of those that a mesh axis runs over, the one named last changes fastest.
Arguments:
- student_hidden: bfloat16 [6912, 3456], P('dp'), may hold values from -6 to 6
- norm_gain: float32 [3456], replicated, may hold values from 0.25 to 1.75
- projection: bfloat16 [3456, 8192], P(None, 'tp'), may hold values from -0.109375 to 0.109375
- teacher_partials: bfloat16 [16, 6912, 8192], P('tp', 'dp'), may hold values from -5 to 5
- teacher_residual: bfloat16 [6912, 8192], P('dp', 'tp'), may hold values from -90 to 90
- owner: int32 [6912], P('dp'), may hold values from 0 to 6911, as said below
Outputs:
- grad_scaled: float32 [3456, 8192], P('dp', 'tp')
The draws below stay inside these ranges and needn't reach their ends.
Inputs may be any that keep to these rules, and one draw needn't show every extreme that they name: owner is a permutation of all token indices; the 144 teacher rows of each index of dp hold exactly 3 tokens owned by each index of dp.
All inputs are finite; a program needn't handle non-finite values.
Results may differ from the reference program's by a relative error of at most 0.009.
Values may be sent and summed in bfloat16 or wider, within the bound.
No kernel may reach another device: no remote copies, remote signals or barrier semaphores. Data moves between devices by JAX's collectives and lax.ppermute only.
A program may use at most 64 MiB of HBM per device.

```python
import jax
import jax.numpy as jnp
from jax import lax

DS = 3456
DTW = 8192
TOK_DEV = 144
TOKENS = 6912
N_DP = 48
N_TP = 16


def draw_owner(key, part):
    blocks = TOKENS // TOK_DEV
    slots = TOK_DEV // blocks
    keys = jax.random.split(jax.random.fold_in(key, 17), 2 * blocks)
    source_perms = jax.vmap(lambda k: jax.random.permutation(k, TOK_DEV))(keys[:blocks])
    target_perms = jax.vmap(lambda k: jax.random.permutation(k, TOK_DEV))(keys[blocks:])
    dest = source_perms // slots
    within = source_perms % slots
    column = jnp.arange(blocks, dtype=jnp.int32)[:, None] * slots + within
    local = target_perms[dest, column]
    return (dest * TOK_DEV + local).reshape(-1).astype(jnp.int32)


def draw_teacher_residual(key, part):
    first, second, third = jax.random.split(jax.random.fold_in(key, 29), 3)
    row_pos = jnp.arange(TOKENS, dtype=jnp.float32) / TOKENS
    col_pos = jnp.arange(DTW, dtype=jnp.float32) / DTW
    row_jitter = jnp.exp(jax.random.uniform(second, (TOKENS,), jnp.float32, -0.3, 0.3))
    col_jitter = jnp.exp(jax.random.uniform(third, (DTW,), jnp.float32, -0.3, 0.3))
    base = jnp.clip(jax.random.normal(first, (TOKENS, DTW), jnp.float32), -4.0, 4.0)
    row_scale = 0.2 * 20.0 ** row_pos * row_jitter
    col_scale = 3.0 ** col_pos * col_jitter
    return (base * row_scale[:, None] * col_scale[None, :]).astype(jnp.bfloat16)


def spiked(array, key, source, target, parts, factor):
    def block_of(dim):
        return (jnp.arange(array.shape[dim]) // (array.shape[dim] // parts)).reshape((-1,) + (1,) * (array.ndim - 1 - dim))

    one_side = jax.random.permutation(key, parts)[block_of(target)]
    other_side = (block_of(target) + parts // 2) % parts
    return jnp.where((block_of(source) == one_side) | (block_of(source) == other_side), factor * array, array)


def steps_of(stream_key, dims, pieces, low, largest):
    def one(axis_at, parts):
        draws = jax.random.uniform(jax.random.fold_in(jax.random.fold_in(stream_key, 6), axis_at), (parts,), jnp.float32, low / len(pieces), largest / len(pieces))
        return jnp.repeat(jnp.exp(draws), dims[axis_at] // parts).reshape((-1,) + (1,) * (len(dims) - axis_at - 1))

    factor_of = one(*pieces[0])
    for cut in pieces[1:]:
        factor_of = factor_of * one(*cut)
    return factor_of


def gaussian(key, shape, scale, most, cuts=(), kind=jnp.bfloat16):
    factor_of = steps_of(key, shape, cuts, -0.22, 0.18) if cuts else 1.0
    array = jax.random.normal(key, shape, jnp.float32) * scale * factor_of
    return jnp.minimum(jnp.maximum(array, -most), most).astype(kind)


def noise_with(stream_key, shape, width, most, shards, heavy, held_as=jnp.bfloat16):
    values = width * jax.random.normal(stream_key, shape, jnp.float32)
    if shards:
        values = values * steps_of(stream_key, shape, shards, -0.22, 0.18)
    return jnp.clip(spiked(values, jax.random.fold_in(stream_key, 3), *heavy), -most, most).astype(held_as)


def setup_inputs(seed: int = 0) -> dict:
    arg_keys = jax.random.split(jax.random.key(seed), 7)
    return {
        "student_hidden": gaussian(arg_keys[0], (TOKENS, DS), 1.0, 6.0, ((0, 48),)),
        "norm_gain": jnp.clip(1.0 + 0.15 * jax.random.normal(arg_keys[1], (DS,), jnp.float32), 0.25, 1.75),
        "projection": gaussian(arg_keys[2], (DS, DTW), DS ** -0.5, 0.109375, ((1, 16),)),
        "teacher_partials": noise_with(arg_keys[3], (N_TP, TOKENS, DTW), 0.25, 5.0, ((0, 16), (1, 48)), (0, 2, 16, 2.0)),
        "teacher_residual": draw_teacher_residual(jax.random.fold_in(arg_keys[6], 71), 0),
        "owner": draw_owner(jax.random.fold_in(arg_keys[6], 71), 0),
    }


def block_partial(pair):
    normed_block, diff_block = pair
    return lax.dot_general(normed_block, diff_block, (((0,), (0,)), ((), ())), preferred_element_type=jnp.float32)

def reference(student_hidden, norm_gain, projection, teacher_partials, teacher_residual, owner):

    def add_rank(index, total):
        return total + lax.dynamic_index_in_dim(teacher_partials, index, 0, keepdims=False).astype(jnp.float32)
    summed = lax.fori_loop(0, N_TP, add_rank, jnp.zeros((TOKENS, DTW), jnp.float32))
    teacher = (teacher_residual.astype(jnp.float32) + summed).astype(jnp.bfloat16)
    target = jnp.zeros((TOKENS, DTW), jnp.bfloat16).at[owner.astype(jnp.int32)].set(teacher)
    values = student_hidden.astype(jnp.float32)
    inverse = lax.rsqrt(lax.optimization_barrier(jnp.mean(values * values, axis=-1, keepdims=True)) + 1e-05)
    normed = (values * inverse * norm_gain).astype(jnp.bfloat16)
    pred = jnp.dot(normed, projection, preferred_element_type=jnp.float32)
    diff = (pred - target.astype(jnp.float32)).astype(jnp.bfloat16)
    normed_blocks = normed.reshape(N_DP, TOK_DEV, DS)
    diff_blocks = diff.reshape(N_DP, TOK_DEV, DTW)
    maxima = lax.map(lambda pair: jnp.max(jnp.abs(block_partial(pair))), (normed_blocks, diff_blocks))
    scale = jnp.max(maxima) + 1e-06

    def accumulate(total, pair):
        rounded = lax.optimization_barrier((block_partial(pair) / scale).astype(jnp.bfloat16))
        return (total + rounded.astype(jnp.float32), None)
    grad_scaled, unused = lax.scan(accumulate, jnp.zeros((DS, DTW), jnp.float32), (normed_blocks, diff_blocks))
    return grad_scaled
```

```python
import jax
import jax.numpy as jnp
from jax import lax
from jax.experimental import pallas as pl
from jax.experimental.pallas import tpu as pltpu
from jax.sharding import Mesh
from jax.sharding import PartitionSpec as P

X, Z, C = "dp_0", "dp_1", "dp_2"
XH, Y = "tp_0", "tp_1"
DP, TP, XC = (X, Z, C), (XH, Y), (X, C)
VMEM = pl.BlockSpec(memory_space=pltpu.VMEM)
SMEM = pl.BlockSpec(memory_space=pltpu.SMEM)
ROWS_FIRST = (((0,), (0,)), ((), ()))
MARKS = 128


def exchange(array, axes):
    return lax.all_to_all(array, axes, split_axis=0, concat_axis=0, tiled=True)


def to_peer(array, k):
    return lax.ppermute(array, XC, [(p, p ^ k) for p in range(4)])


def cost(flops, moved):
    return pl.CostEstimate(flops=flops, bytes_accessed=moved, transcendentals=0)


def split_kernel(in_ref, out_ref):
    out_ref[0] = in_ref[...]


def split_columns(array, parts):
    rows, width = array.shape
    columns = width // parts
    return pl.pallas_call(
        split_kernel,
        out_shape=jax.ShapeDtypeStruct((parts, rows, columns), array.dtype),
        grid=(parts,),
        in_specs=[pl.BlockSpec((rows, columns), lambda k: (0, k))],
        out_specs=pl.BlockSpec((1, rows, columns), lambda k: (k, 0, 0)),
        name="split_columns",
        cost_estimate=cost(0, 4 * rows * width),
    )(array)


def student_kernel(sizes, me_ref, hidden_ref, gain_ref, proj_ref, pred_ref, parts_ref, wide_ref, part_ref):
    nx, nz, nc, block = sizes
    values = hidden_ref[...].astype(jnp.float32)
    inverse = lax.rsqrt(jnp.mean(values * values, axis=-1, keepdims=True) + 1e-05)
    normed = values * inverse * gain_ref[...]
    pred = jnp.dot(normed.astype(jnp.bfloat16), proj_ref[...], preferred_element_type=jnp.float32)
    pred_ref[...] = pred.astype(jnp.bfloat16)
    wide_ref[...] = normed
    for p in range(nx * nc):
        x, c = p // nc, p % nc
        for z in range(nz):
            start = ((x * nz + z) * nc + c) * block
            part_ref[:, z * block : (z + 1) * block] = wide_ref[:, start : start + block]
        parts_ref[p ^ me_ref[0]] = part_ref[...].astype(jnp.bfloat16)


def student(me, hidden, gain, projection, sizes):
    nx, nz, nc, block = sizes
    rows, features = hidden.shape
    columns = projection.shape[1]
    return pl.pallas_call(
        lambda *refs: student_kernel(sizes, *refs),
        out_shape=(
            jax.ShapeDtypeStruct((rows, columns), jnp.bfloat16),
            jax.ShapeDtypeStruct((nx * nc, rows, nz * block), jnp.bfloat16),
        ),
        in_specs=[SMEM, VMEM, VMEM, VMEM],
        out_specs=(VMEM, VMEM),
        scratch_shapes=[
            pltpu.VMEM((rows, features), jnp.float32),
            pltpu.VMEM((rows, nz * block), jnp.float32),
        ],
        name="student",
        cost_estimate=cost(2 * rows * features * columns, 2 * features * columns),
    )(me, hidden, gain, projection)


def teacher_kernel(terms_ref, residual_ref, slot_ref, marks_ref, out_ref):
    count, rows, columns = terms_ref.shape
    summed = terms_ref[0].astype(jnp.float32)
    for k in range(1, count):
        summed = summed + terms_ref[k].astype(jnp.float32)
    teacher = (residual_ref[...].astype(jnp.float32) + summed).astype(jnp.bfloat16)
    lanes = lax.broadcasted_iota(jnp.int32, (rows, out_ref.shape[0]), 1)
    select = (lanes == slot_ref[...]).astype(jnp.float32).astype(jnp.bfloat16)
    for at, part in ((0, teacher), (columns, marks_ref[...])):
        moved = lax.dot_general(select, part, ROWS_FIRST, preferred_element_type=jnp.float32)
        out_ref[:, at : at + part.shape[1]] = moved.astype(jnp.bfloat16)


def teacher_rows(terms, residual, slot, marks, slots):
    rows, columns = residual.shape
    return pl.pallas_call(
        teacher_kernel,
        out_shape=jax.ShapeDtypeStruct((slots, columns + MARKS), jnp.bfloat16),
        in_specs=[VMEM] * 4,
        out_specs=VMEM,
        name="teacher_rows",
        cost_estimate=cost(2 * rows * columns * slots, 2 * terms.size),
    )(terms, residual, slot, marks)


def gradient_kernel(me_ref, rows_ref, pred_ref, normed_ref, sum_ref, max_ref):
    groups, per, height = normed_ref.shape
    columns = pred_ref.shape[-1]
    peer = rows_ref[:, columns : columns + 1].astype(jnp.float32).astype(jnp.int32)
    local = rows_ref[:, columns + 1 : columns + 2].astype(jnp.float32).astype(jnp.int32)
    place = (peer ^ me_ref[0]) * per + local
    lanes = lax.broadcasted_iota(jnp.int32, (rows_ref.shape[0], groups * per), 1)
    select = (lanes == place).astype(jnp.float32).astype(jnp.bfloat16)
    target = lax.dot_general(
        select, rows_ref[:, :columns], ROWS_FIRST, preferred_element_type=jnp.float32
    )
    largest = jnp.zeros((1, 1), jnp.float32)
    total = None
    for g in range(groups):
        aimed = target[g * per : (g + 1) * per]
        diff = (pred_ref[g].astype(jnp.float32) - aimed).astype(jnp.bfloat16)
        part = lax.dot_general(normed_ref[g], diff, ROWS_FIRST, preferred_element_type=jnp.float32)
        largest = jnp.maximum(largest, jnp.max(jnp.abs(part), keepdims=True))
        total = part if total is None else total + part
    sum_ref[...] = total.astype(jnp.bfloat16)
    max_ref[...] = jnp.broadcast_to(largest, max_ref.shape)


def gradient(me, rows, pred, normed):
    groups, per, height = normed.shape
    columns = pred.shape[-1]
    return pl.pallas_call(
        gradient_kernel,
        out_shape=(
            jax.ShapeDtypeStruct((height, columns), jnp.bfloat16),
            jax.ShapeDtypeStruct((8, 128), jnp.float32),
        ),
        in_specs=[SMEM, VMEM, VMEM, VMEM],
        out_specs=(VMEM, VMEM),
        name="gradient",
        cost_estimate=cost(4 * groups * per * height * columns, 4 * normed.size),
    )(me, rows, pred, normed)


def per_device(student_hidden, norm_gain, projection, teacher_partials, teacher_residual, owner):
    rows_dev, columns = teacher_residual.shape
    features = student_hidden.shape[1]
    nx, nz, nc = (lax.axis_size(a) for a in DP)
    peers = nx * nc
    block = features // (nx * nz * nc)
    per_z = rows_dev // nz
    slots_z = -(-per_z // 16) * 16
    me = lax.axis_index(X) * nc + lax.axis_index(C)
    me_ref = me.reshape(1).astype(jnp.int32)

    with jax.named_scope("terms"):
        terms = exchange(split_columns(teacher_partials[0], lax.axis_size(TP)), TP)

    with jax.named_scope("student"):
        sizes = (nx, nz, nc, block)
        pred, parts = student(me_ref, student_hidden, norm_gain[None], projection, sizes)
        pred_parts = [pred] + [to_peer(pred, k) for k in range(1, peers)]
        normed_parts = [parts[0]] + [to_peer(parts[k], k) for k in range(1, peers)]
        pred_all, normed_all = jnp.stack(pred_parts), jnp.stack(normed_parts)

    with jax.named_scope("places"):
        whose = owner // rows_dev
        z_to = (whose // nc) % nz
        peer_to = (whose // (nz * nc)) * nc + whose % nc
        index = jnp.arange(rows_dev)
        earlier = (z_to[None, :] == z_to[:, None]) & (index[None, :] < index[:, None])
        slot = z_to * slots_z + jnp.sum(earlier.astype(jnp.int32), axis=1)
        lane = lax.broadcasted_iota(jnp.int32, (rows_dev, MARKS), 1)
        marks = jnp.where(lane == 0, peer_to[:, None], (owner % rows_dev)[:, None])
        marks = jnp.where(lane < 2, marks, 0).astype(jnp.bfloat16)
        slot = slot[:, None]

    terms, pred_all, normed_all, slot, marks = lax.optimization_barrier(
        (terms, pred_all, normed_all, slot, marks)
    )

    with jax.named_scope("regroup"):
        outgoing = teacher_rows(terms, teacher_residual, slot, marks, nz * slots_z)
        arrived = exchange(outgoing.reshape(nz, slots_z, -1), Z).reshape(nz * slots_z, -1)
        rows = lax.all_gather(arrived, XC, axis=0, tiled=True)

    with jax.named_scope("grad"):
        tile, largest = gradient(me_ref, rows, pred_all, normed_all)
        pieces = exchange(tile.reshape(nz, block, columns), Z)
        scale = jnp.max(largest)
        for axis in (C, X, XH, Y, Z):
            scale = lax.pmax(scale, axis)
        scale = scale + 1e-06
        return jnp.sum(pieces.astype(jnp.float32), axis=0) / scale


def solution(mesh):
    torus = Mesh(mesh.devices.reshape(2, 12, 2, 2, 8), (X, Z, C, XH, Y))
    placed = (P(DP, None), P(), P(None, TP), P(TP, DP, None), P(DP, TP), P(DP))
    return jax.shard_map(
        per_device, mesh=torus, in_specs=placed, out_specs=P(DP, TP), check_vma=False
    )
```

```python
import jax
import jax.numpy as jnp
from jax import lax
from jax.experimental import pallas as pl
from jax.experimental.pallas import tpu as pltpu
from jax.sharding import Mesh
from jax.sharding import PartitionSpec as P

X, ZH, ZL, C = "x_lo", "z_hi", "z_lo", "core"
XH, Y = "x_hi", "y"
DP, TP, XC, Z = (X, ZH, ZL, C), (XH, Y), (X, C), (ZH, ZL)
VMEM = pl.BlockSpec(memory_space=pltpu.VMEM)
SMEM = pl.BlockSpec(memory_space=pltpu.SMEM)
ROWS_FIRST = (((0,), (0,)), ((), ()))
MARKS, FULL, REST = 128, 8, 4


def exchange(array, axes):
    return lax.all_to_all(array, axes, split_axis=0, concat_axis=0, tiled=True)


def to_peer(array, k):
    return lax.ppermute(array, XC, [(p, p ^ k) for p in range(4)])


def cost(flops, moved):
    return pl.CostEstimate(flops=flops, bytes_accessed=moved, transcendentals=0)


def split_kernel(in_ref, out_ref):
    parts, _, columns = out_ref.shape
    for k in range(parts):
        out_ref[k] = in_ref[:, k * columns : (k + 1) * columns]


def split_columns(array, parts):
    rows, width = array.shape
    return pl.pallas_call(
        split_kernel,
        out_shape=jax.ShapeDtypeStruct((parts, rows, width // parts), array.dtype),
        in_specs=[VMEM],
        out_specs=VMEM,
        name="split_columns",
        cost_estimate=cost(0, 4 * rows * width),
    )(array)


def student_kernel(sizes, me_ref, hidden_ref, gain_ref, proj_ref, pred_ref, parts_ref, wide_ref, part_ref):
    nx, nz, nc, block = sizes
    values = hidden_ref[...].astype(jnp.float32)
    inverse = lax.rsqrt(jnp.mean(values * values, axis=-1, keepdims=True) + 1e-05)
    normed = values * inverse * gain_ref[...]
    pred = jnp.dot(normed.astype(jnp.bfloat16), proj_ref[...], preferred_element_type=jnp.float32)
    pred_ref[...] = pred.astype(jnp.bfloat16)
    wide_ref[...] = normed
    for p in range(nx * nc):
        x, c = p // nc, p % nc
        for z in range(nz):
            start = ((x * nz + z) * nc + c) * block
            part_ref[:, z * block : (z + 1) * block] = wide_ref[:, start : start + block]
        parts_ref[p ^ me_ref[0]] = part_ref[...].astype(jnp.bfloat16)


def student(me, hidden, gain, projection, sizes):
    nx, nz, nc, block = sizes
    rows, features = hidden.shape
    columns = projection.shape[1]
    return pl.pallas_call(
        lambda *refs: student_kernel(sizes, *refs),
        out_shape=(
            jax.ShapeDtypeStruct((rows, columns), jnp.bfloat16),
            jax.ShapeDtypeStruct((nx * nc, rows, nz * block), jnp.bfloat16),
        ),
        in_specs=[SMEM, VMEM, VMEM, VMEM],
        out_specs=(VMEM, VMEM),
        scratch_shapes=[
            pltpu.VMEM((rows, features), jnp.float32),
            pltpu.VMEM((rows, nz * block), jnp.float32),
        ],
        name="student",
        cost_estimate=cost(2 * rows * features * columns, 2 * features * columns),
    )(me, hidden, gain, projection)


def teacher_kernel(terms_ref, residual_ref, slots_ref, marks_ref, out_ref):
    count, rows, columns = terms_ref.shape
    half = columns // 2
    summed = terms_ref[0].astype(jnp.float32)
    for k in range(1, count):
        summed = summed + terms_ref[k].astype(jnp.float32)
    teacher = (residual_ref[...].astype(jnp.float32) + summed).astype(jnp.bfloat16)
    lines = lax.broadcasted_iota(jnp.int32, (out_ref.shape[0], rows), 0)
    full, low, high = (
        (lines == slots_ref[k : k + 1, :]).astype(jnp.float32).astype(jnp.bfloat16) for k in range(3)
    )

    def moved(select, part):
        return jnp.dot(select, part, preferred_element_type=jnp.float32)

    rest = moved(low, teacher[:, :half]) + moved(high, teacher[:, half:])
    out_ref[:, :columns] = moved(full, teacher).astype(jnp.bfloat16)
    out_ref[:, columns : columns + half] = rest.astype(jnp.bfloat16)
    out_ref[:, columns + half :] = moved(full + low + high, marks_ref[...]).astype(jnp.bfloat16)


def teacher_rows(terms, residual, slots, marks, lines):
    rows, columns = residual.shape
    width = columns + columns // 2 + MARKS
    return pl.pallas_call(
        teacher_kernel,
        out_shape=jax.ShapeDtypeStruct((lines, width), jnp.bfloat16),
        in_specs=[VMEM] * 4,
        out_specs=VMEM,
        name="teacher_rows",
        cost_estimate=cost(2 * rows * width * lines, 2 * terms.size),
    )(terms, residual, slots, marks)


def gradient_kernel(me_ref, rows_ref, pred_ref, normed_ref, sum_ref, max_ref):
    groups, per, height = normed_ref.shape
    columns = pred_ref.shape[-1]
    half = columns // 2
    lines, tokens = rows_ref.shape[0], groups * per
    marks = rows_ref[:, columns + half :].astype(jnp.float32).astype(jnp.int32)
    lanes = lax.broadcasted_iota(jnp.int32, (lines, tokens), 1)
    line = lax.broadcasted_iota(jnp.int32, (lines, tokens), 0)
    low_half = (line & (FULL - 1)) < REST

    def select(at, wanted):
        place = (marks[:, at : at + 1] ^ me_ref[0]) * per + marks[:, at + 1 : at + 2]
        return ((lanes == place) & wanted).astype(jnp.float32).astype(jnp.bfloat16)

    def placed(chosen, start):
        return lax.dot_general(
            chosen, rows_ref[:, start : start + half], ROWS_FIRST, preferred_element_type=jnp.float32
        )

    full = select(0, True)
    target = [
        placed(full, 0) + placed(select(2, low_half), columns),
        placed(full, half) + placed(select(2, ~low_half), columns),
    ]
    largest = jnp.zeros((1, 1), jnp.float32)
    for side in range(2):
        cols = slice(side * half, (side + 1) * half)
        total = None
        for g in range(groups):
            aimed = target[side][g * per : (g + 1) * per]
            diff = (pred_ref[g, :, cols].astype(jnp.float32) - aimed).astype(jnp.bfloat16)
            part = lax.dot_general(normed_ref[g], diff, ROWS_FIRST, preferred_element_type=jnp.float32)
            largest = jnp.maximum(largest, jnp.max(jnp.abs(part), keepdims=True))
            total = part if total is None else total + part
        sum_ref[:, cols] = total.astype(jnp.bfloat16)
    max_ref[0, 0] = jnp.max(largest)


def gradient(me, rows, pred, normed):
    groups, per, height = normed.shape
    columns = pred.shape[-1]
    return pl.pallas_call(
        gradient_kernel,
        out_shape=(
            jax.ShapeDtypeStruct((height, columns), jnp.bfloat16),
            jax.ShapeDtypeStruct((1, 1), jnp.float32),
        ),
        in_specs=[SMEM, VMEM, VMEM, VMEM],
        out_specs=(VMEM, SMEM),
        name="gradient",
        cost_estimate=cost(4 * groups * per * height * columns, 4 * normed.size),
    )(me, rows, pred, normed)


def per_device(student_hidden, norm_gain, projection, teacher_partials, teacher_residual, owner):
    rows_dev, columns = teacher_residual.shape
    features = student_hidden.shape[1]
    nx, nz, nc = (lax.axis_size(a) for a in (X, Z, C))
    peers = nx * nc
    block = features // (nx * nz * nc)
    assert rows_dev == nz * (FULL + REST)
    me = lax.axis_index(X) * nc + lax.axis_index(C)
    me_ref = me.reshape(1).astype(jnp.int32)

    with jax.named_scope("terms"):
        terms = exchange(split_columns(teacher_partials[0], lax.axis_size(TP)), TP)

    with jax.named_scope("student"):
        sizes = (nx, nz, nc, block)
        pred, parts = student(me_ref, student_hidden, norm_gain[None], projection, sizes)
        pred_parts = [pred] + [to_peer(pred, k) for k in range(1, peers)]
        normed_parts = [parts[0]] + [to_peer(parts[k], k) for k in range(1, peers)]
        pred_all, normed_all = jnp.stack(pred_parts), jnp.stack(normed_parts)

    with jax.named_scope("places"):
        whose = owner // rows_dev
        z_to = (whose // nc) % nz
        peer_to = (whose // (nz * nc)) * nc + whose % nc
        index = jnp.arange(rows_dev)
        earlier = (z_to[None, :] == z_to[:, None]) & (index[None, :] < index[:, None])
        rank = jnp.sum(earlier.astype(jnp.int32), axis=1)
        full = rank < FULL
        line = z_to * FULL + jnp.where(full, rank, rank - FULL)
        slots = jnp.stack([jnp.where(full, line, -1), jnp.where(full, -1, line)])
        slots = jnp.concatenate([slots, jnp.where(full, -1, line + REST)[None]])
        lane = lax.broadcasted_iota(jnp.int32, (rows_dev, MARKS), 1) - jnp.where(full, 0, 2)[:, None]
        marks = jnp.where(lane == 0, peer_to[:, None], (owner % rows_dev)[:, None])
        marks = jnp.where((lane == 0) | (lane == 1), marks, 0).astype(jnp.bfloat16)

    terms, pred_all, normed_all = lax.optimization_barrier((terms, pred_all, normed_all))

    with jax.named_scope("regroup"):
        outgoing = teacher_rows(terms, teacher_residual, slots, marks, nz * FULL)
        arrived = exchange(outgoing.reshape(nz, FULL, -1), Z).reshape(nz * FULL, -1)
        rows = lax.all_gather(arrived, XC, axis=0, tiled=True)

    with jax.named_scope("grad"):
        tile, largest = gradient(me_ref, rows, pred_all, normed_all)
        pieces = exchange(tile.reshape(nz, block, columns), Z)
        scale = largest[0, 0]
        for axes in (C, (XH, X), Y, ZL, ZH):
            scale = lax.pmax(scale, axes)
        scale = scale + 1e-06
        return jnp.sum(pieces.astype(jnp.float32), axis=0) / scale


def solution(mesh):
    torus = Mesh(mesh.devices.reshape(2, 3, 4, 2, 2, 8), (X, ZH, ZL, C, XH, Y))
    placed = (P(DP, None), P(), P(None, TP), P(TP, DP, None), P(DP, TP), P(DP))
    return jax.shard_map(
        per_device, mesh=torus, in_specs=placed, out_specs=P(DP, TP), check_vma=False
    )
```

```python
import jax
import jax.numpy as jnp
from jax import lax
from jax.experimental import pallas as pl
from jax.experimental.pallas import tpu as pltpu
from jax.sharding import Mesh
from jax.sharding import PartitionSpec as P


X, ZH, ZL, C = "x_lo", "z_hi", "z_lo", "core"
XH, Y = "x_hi", "y"
DP, TP, XC, Z = (X, ZH, ZL, C), (XH, Y), (X, C), (ZH, ZL)
VMEM = pl.BlockSpec(memory_space=pltpu.VMEM)
SMEM = pl.BlockSpec(memory_space=pltpu.SMEM)
ROWS_FIRST = (((0,), (0,)), ((), ()))
MARKS, FULL, REST = 128, 8, 4


def exchange(array, axes):
    return lax.all_to_all(array, axes, split_axis=0, concat_axis=0, tiled=True)


def to_peer(array, k):
    return lax.ppermute(array, XC, [(p, p ^ k) for p in range(4)])


def cost(flops, moved):
    return pl.CostEstimate(flops=flops, bytes_accessed=moved, transcendentals=0)


def half_of(array):
    return pl.BlockSpec((array.shape[0], array.shape[1] // 2), lambda _, which: (0, which[0]))


def pieces_of(columns):
    return ((0, columns // 4), (columns // 4, columns))


def split_kernel(_, in_ref, *out_refs):
    columns = sum(ref.shape[-1] for ref in out_refs)
    for ref, (start, stop) in zip(out_refs, pieces_of(columns)):
        for k in range(ref.shape[0]):
            ref[k] = in_ref[:, k * columns + start : k * columns + stop]


def split_columns(which, array, parts, columns):
    rows = array.shape[0]
    shapes = [(parts, rows, stop - start) for start, stop in pieces_of(columns)]
    return pl.pallas_call(
        split_kernel,
        out_shape=[jax.ShapeDtypeStruct(shape, array.dtype) for shape in shapes],
        grid_spec=pltpu.PrefetchScalarGridSpec(
            num_scalar_prefetch=1,
            grid=(1,),
            in_specs=[half_of(array)],
            out_specs=[pl.BlockSpec(shape, lambda *_: (0, 0, 0)) for shape in shapes],
        ),
        name="split_columns",
        cost_estimate=cost(0, 2 * array.size),
    )(which, array)


def pair_kernel(start, columns, _, in_ref, got_ref, out_ref):
    width = got_ref.shape[-1]
    for k in range(got_ref.shape[0]):
        at = k * columns + start
        mine = in_ref[:, at : at + width].astype(jnp.float32)
        out_ref[k] = (mine + got_ref[k].astype(jnp.float32)).astype(jnp.bfloat16)


def pair_sum(which, array, got, start, columns):
    return pl.pallas_call(
        lambda *refs: pair_kernel(start, columns, *refs),
        out_shape=jax.ShapeDtypeStruct(got.shape, got.dtype),
        grid_spec=pltpu.PrefetchScalarGridSpec(
            num_scalar_prefetch=1,
            grid=(1,),
            in_specs=[half_of(array), pl.BlockSpec(got.shape, lambda *_: (0, 0, 0))],
            out_specs=pl.BlockSpec(got.shape, lambda *_: (0, 0, 0)),
        ),
        name="pair_sum",
        cost_estimate=cost(got.size, 6 * got.size),
    )(which, array, got)


def lane_tiles(width):
    return -(-width // 128) * 128


def student_kernel(sizes, me_ref, hidden_ref, gain_ref, proj_ref, *refs):
    nx, nz, nc, block = sizes
    peers = nx * nc
    out_refs, (wide_ref, line_ref, parts_ref) = refs[:peers], refs[peers:]
    values = hidden_ref[...].astype(jnp.float32)
    inverse = lax.rsqrt(jnp.mean(values * values, axis=-1, keepdims=True) + 1e-05)
    normed = values * inverse * gain_ref[...]
    pred = jnp.dot(normed.astype(jnp.bfloat16), proj_ref[...], preferred_element_type=jnp.float32)
    pred = pred.astype(jnp.bfloat16)
    wide_ref[...] = normed
    line_ref[...] = jnp.zeros_like(line_ref)
    for p in range(peers):
        x, c = p // nc, p % nc
        for z in range(nz):
            start = ((x * nz + z) * nc + c) * block
            line_ref[:, z * block : (z + 1) * block] = wide_ref[:, start : start + block]
        parts_ref[p] = line_ref[...].astype(jnp.bfloat16)
    at = line_ref.shape[-1]
    for k in range(peers):
        out_refs[k][:, :at] = parts_ref[me_ref[0] ^ k]
        out_refs[k][:, at:] = pred


def student(me, hidden, gain, projection, sizes):
    nx, nz, nc, block = sizes
    rows, features = hidden.shape
    columns = projection.shape[1]
    peers, wide = nx * nc, lane_tiles(nz * block)
    return pl.pallas_call(
        lambda *refs: student_kernel(sizes, *refs),
        out_shape=[jax.ShapeDtypeStruct((rows, wide + columns), jnp.bfloat16)] * peers,
        in_specs=[SMEM, VMEM, VMEM, VMEM],
        out_specs=[VMEM] * peers,
        scratch_shapes=[
            pltpu.VMEM((rows, features), jnp.float32),
            pltpu.VMEM((rows, wide), jnp.float32),
            pltpu.VMEM((peers, rows, wide), jnp.bfloat16),
        ],
        name="student",
        cost_estimate=cost(2 * rows * features * columns, 2 * features * columns),
    )(me, hidden, gain, projection)


def teacher_kernel(first_ref, second_ref, residual_ref, slots_ref, marks_ref, out_ref):
    rows, columns = residual_ref.shape
    half = columns // 2
    sums = []
    for terms_ref in (first_ref, second_ref):
        total = terms_ref[0].astype(jnp.float32)
        for k in range(1, terms_ref.shape[0]):
            total = total + terms_ref[k].astype(jnp.float32)
        sums.append(total)
    summed = jnp.concatenate(sums, axis=1)
    teacher = (residual_ref[...].astype(jnp.float32) + summed).astype(jnp.bfloat16)
    lines = lax.broadcasted_iota(jnp.int32, (out_ref.shape[0], rows), 0)
    full, low, high = (
        (lines == slots_ref[k : k + 1, :]).astype(jnp.float32).astype(jnp.bfloat16) for k in range(3)
    )

    def moved(select, part):
        return jnp.dot(select, part, preferred_element_type=jnp.float32)

    rest = moved(low, teacher[:, :half]) + moved(high, teacher[:, half:])
    out_ref[:, :columns] = moved(full, teacher).astype(jnp.bfloat16)
    out_ref[:, columns : columns + half] = rest.astype(jnp.bfloat16)
    out_ref[:, columns + half :] = moved(full + low + high, marks_ref[...]).astype(jnp.bfloat16)


def teacher_rows(first, second, residual, slots, marks, lines):
    rows, columns = residual.shape
    width = columns + columns // 2 + MARKS
    return pl.pallas_call(
        teacher_kernel,
        out_shape=jax.ShapeDtypeStruct((lines, width), jnp.bfloat16),
        in_specs=[VMEM] * 5,
        out_specs=VMEM,
        name="teacher_rows",
        cost_estimate=cost(2 * rows * width * lines, 16 * residual.size),
    )(first, second, residual, slots, marks)


def gradient_kernel(me_ref, rows_ref, *refs):
    student_refs, (sum_ref, max_ref) = refs[:-2], refs[-2:]
    height, columns = sum_ref.shape
    groups, per = len(student_refs), student_refs[0].shape[0]
    pred_at = lane_tiles(height)
    half = columns // 2
    lines, tokens = rows_ref.shape[0], groups * per
    marks = rows_ref[:, columns + half :].astype(jnp.float32).astype(jnp.int32)
    lanes = lax.broadcasted_iota(jnp.int32, (lines, tokens), 1)
    line = lax.broadcasted_iota(jnp.int32, (lines, tokens), 0)
    low_half = (line & (FULL - 1)) < REST

    def select(at, wanted):
        place = (marks[:, at : at + 1] ^ me_ref[0]) * per + marks[:, at + 1 : at + 2]
        return ((lanes == place) & wanted).astype(jnp.float32).astype(jnp.bfloat16)

    def placed(chosen, start):
        return lax.dot_general(
            chosen, rows_ref[:, start : start + half], ROWS_FIRST, preferred_element_type=jnp.float32
        )

    full = select(0, True)
    target = [
        placed(full, 0) + placed(select(2, low_half), columns),
        placed(full, half) + placed(select(2, ~low_half), columns),
    ]
    largest = jnp.zeros((1, 1), jnp.float32)
    for side in range(2):
        cols = slice(side * half, (side + 1) * half)
        total = None
        for g, ref in enumerate(student_refs):
            aimed = target[side][g * per : (g + 1) * per]
            pred = ref[:, pred_at + side * half : pred_at + (side + 1) * half]
            diff = (pred.astype(jnp.float32) - aimed).astype(jnp.bfloat16)
            part = lax.dot_general(
                ref[:, :height], diff, ROWS_FIRST, preferred_element_type=jnp.float32
            )
            largest = jnp.maximum(largest, jnp.max(jnp.abs(part), keepdims=True))
            total = part if total is None else total + part
        sum_ref[:, cols] = total.astype(jnp.bfloat16)
    max_ref[0, 0] = jnp.max(largest)


def gradient(me, rows, packed, height, columns):
    tokens = len(packed) * packed[0].shape[0]
    return pl.pallas_call(
        gradient_kernel,
        out_shape=(
            jax.ShapeDtypeStruct((height, columns), jnp.bfloat16),
            jax.ShapeDtypeStruct((1, 1), jnp.float32),
        ),
        in_specs=[SMEM, VMEM] + [VMEM] * len(packed),
        out_specs=(VMEM, SMEM),
        name="gradient",
        cost_estimate=cost(4 * tokens * height * columns, 4 * tokens * height),
    )(me, rows, *packed)


def per_device(student_hidden, norm_gain, projection, teacher_partials, teacher_residual, owner):
    rows_dev, columns = teacher_residual.shape
    features = student_hidden.shape[1]
    nx, nz, nc = (lax.axis_size(a) for a in (X, Z, C))
    peers = nx * nc
    block = features // (nx * nz * nc)
    assert rows_dev == nz * (FULL + REST)
    me = lax.axis_index(X) * nc + lax.axis_index(C)
    me_ref = me.reshape(1).astype(jnp.int32)

    partner = [(0, 1), (1, 0)]
    here = lax.axis_index(XH).reshape(1).astype(jnp.int32)
    own_terms = teacher_partials[0]
    starts = [start for start, _ in pieces_of(columns)]
    away = split_columns(1 - here, own_terms, lax.axis_size(Y), columns)
    early = lax.ppermute(away[0], XH, partner)
    late = lax.ppermute(away[1], XH, partner)

    packed = student(me_ref, student_hidden, norm_gain[None], projection, (nx, nz, nc, block))
    early = pair_sum(here, own_terms, early, starts[0], columns)
    early, packed = lax.optimization_barrier((early, packed))
    packed = [packed[0]] + [to_peer(packed[k], k) for k in range(1, peers)]
    first = exchange(early, (Y,))
    first, late = lax.optimization_barrier((first, late))
    late = pair_sum(here, own_terms, late, starts[1], columns)
    second = exchange(late, (Y,))

    whose = owner // rows_dev
    z_to = (whose // nc) % nz
    peer_to = (whose // (nz * nc)) * nc + whose % nc
    index = jnp.arange(rows_dev)
    earlier = (z_to[None, :] == z_to[:, None]) & (index[None, :] < index[:, None])
    rank = jnp.sum(earlier.astype(jnp.int32), axis=1)
    full = rank < FULL
    line = z_to * FULL + jnp.where(full, rank, rank - FULL)
    slots = jnp.stack([jnp.where(full, line, -1), jnp.where(full, -1, line)])
    slots = jnp.concatenate([slots, jnp.where(full, -1, line + REST)[None]])
    lane = lax.broadcasted_iota(jnp.int32, (rows_dev, MARKS), 1) - jnp.where(full, 0, 2)[:, None]
    marks = jnp.where(lane == 0, peer_to[:, None], (owner % rows_dev)[:, None])
    marks = jnp.where((lane == 0) | (lane == 1), marks, 0).astype(jnp.bfloat16)

    second, packed = lax.optimization_barrier((second, packed))

    outgoing = teacher_rows(first, second, teacher_residual, slots, marks, nz * FULL)
    arrived = exchange(outgoing.reshape(nz, FULL, -1), Z).reshape(nz * FULL, -1)
    rows = lax.all_gather(arrived, XC, axis=0, tiled=True)

    tile, largest = gradient(me_ref, rows, packed, nz * block, columns)
    pieces = exchange(tile.reshape(nz, block, columns), Z)
    scale = largest[0, 0]
    for axes in (C, (XH, X), Y, ZL, ZH):
        scale = lax.pmax(scale, axes)
    scale = scale + 1e-06
    return jnp.sum(pieces.astype(jnp.float32), axis=0) / scale


def solution(mesh):
    torus = Mesh(mesh.devices.reshape(2, 3, 4, 2, 2, 8), (X, ZH, ZL, C, XH, Y))
    placed = (P(DP, None), P(), P(None, TP), P(TP, DP, None), P(DP, TP), P(DP))
    return jax.shard_map(
        per_device, mesh=torus, in_specs=placed, out_specs=P(DP, TP), check_vma=False
    )
```

```python
import jax
import jax.numpy as jnp
from jax import lax
from jax.experimental import pallas as pl
from jax.experimental.pallas import tpu as pltpu
from jax.sharding import Mesh
from jax.sharding import PartitionSpec as P


X, ZH, ZL, C = "x_lo", "z_hi", "z_lo", "core"
XH, Y = "x_hi", "y"
DP, TP, XC, Z = (X, ZH, ZL, C), (XH, Y), (X, C), (ZH, ZL)
VMEM = pl.BlockSpec(memory_space=pltpu.VMEM)
SMEM = pl.BlockSpec(memory_space=pltpu.SMEM)
ROWS_FIRST = (((0,), (0,)), ((), ()))
MARKS, FULL, REST = 128, 8, 4


def exchange(array, axes):
    return lax.all_to_all(array, axes, split_axis=0, concat_axis=0, tiled=True)


def to_peer(array, k):
    return lax.ppermute(array, XC, [(p, p ^ k) for p in range(4)])


def cost(flops, moved):
    return pl.CostEstimate(flops=flops, bytes_accessed=moved, transcendentals=0)


def half_of(array):
    return pl.BlockSpec((array.shape[0], array.shape[1] // 2), lambda _, which: (0, which[0]))


def direct_kernel(in_ref, out_ref):
    parts, _, width = out_ref.shape
    for k in range(parts):
        out_ref[k] = in_ref[:, 2 * k * width : (2 * k + 1) * width]


def direct_columns(array, parts):
    rows, width = array.shape
    half = width // parts // 2
    return pl.pallas_call(
        direct_kernel,
        out_shape=jax.ShapeDtypeStruct((parts, rows, half), array.dtype),
        in_specs=[VMEM],
        out_specs=VMEM,
        name="direct_columns",
        cost_estimate=cost(0, 3 * array.size),
    )(array)


def away_kernel(_, in_ref, out_ref):
    parts, _, width = out_ref.shape
    for k in range(parts):
        out_ref[k] = in_ref[:, (2 * k + 1) * width : 2 * (k + 1) * width]


def away_columns(which, array, parts):
    rows, width = array.shape
    shape = (parts, rows, width // parts // 4)
    return pl.pallas_call(
        away_kernel,
        out_shape=jax.ShapeDtypeStruct(shape, array.dtype),
        grid_spec=pltpu.PrefetchScalarGridSpec(
            num_scalar_prefetch=1,
            grid=(1,),
            in_specs=[half_of(array)],
            out_specs=pl.BlockSpec(shape, lambda *_: (0, 0, 0)),
        ),
        name="away_columns",
        cost_estimate=cost(0, 2 * array.size),
    )(which, array)


def pair_kernel(_, in_ref, got_ref, out_ref):
    parts, _, width = got_ref.shape
    for k in range(parts):
        mine = in_ref[:, (2 * k + 1) * width : 2 * (k + 1) * width].astype(jnp.float32)
        out_ref[k] = (mine + got_ref[k].astype(jnp.float32)).astype(jnp.bfloat16)


def pair_sum(which, array, got):
    return pl.pallas_call(
        pair_kernel,
        out_shape=jax.ShapeDtypeStruct(got.shape, got.dtype),
        grid_spec=pltpu.PrefetchScalarGridSpec(
            num_scalar_prefetch=1,
            grid=(1,),
            in_specs=[half_of(array), pl.BlockSpec(got.shape, lambda *_: (0, 0, 0))],
            out_specs=pl.BlockSpec(got.shape, lambda *_: (0, 0, 0)),
        ),
        name="pair_sum",
        cost_estimate=cost(got.size, 6 * got.size),
    )(which, array, got)


def lane_tiles(width):
    return -(-width // 128) * 128


def student_kernel(sizes, me_ref, hidden_ref, gain_ref, proj_ref, *refs):
    nx, nz, nc, block = sizes
    peers = nx * nc
    out_refs, (wide_ref, line_ref, parts_ref) = refs[:peers], refs[peers:]
    values = hidden_ref[...].astype(jnp.float32)
    inverse = lax.rsqrt(jnp.mean(values * values, axis=-1, keepdims=True) + 1e-05)
    normed = values * inverse * gain_ref[...]
    pred = jnp.dot(normed.astype(jnp.bfloat16), proj_ref[...], preferred_element_type=jnp.float32)
    pred = pred.astype(jnp.bfloat16)
    wide_ref[...] = normed
    line_ref[...] = jnp.zeros_like(line_ref)
    for p in range(peers):
        x, c = p // nc, p % nc
        for z in range(nz):
            start = ((x * nz + z) * nc + c) * block
            line_ref[:, z * block : (z + 1) * block] = wide_ref[:, start : start + block]
        parts_ref[p] = line_ref[...].astype(jnp.bfloat16)
    at = line_ref.shape[-1]
    for k in range(peers):
        out_refs[k][:, :at] = parts_ref[me_ref[0] ^ k]
        out_refs[k][:, at:] = pred


def student(me, hidden, gain, projection, sizes):
    nx, nz, nc, block = sizes
    rows, features = hidden.shape
    columns = projection.shape[1]
    peers, wide = nx * nc, lane_tiles(nz * block)
    return pl.pallas_call(
        lambda *refs: student_kernel(sizes, *refs),
        out_shape=[jax.ShapeDtypeStruct((rows, wide + columns), jnp.bfloat16)] * peers,
        in_specs=[SMEM, VMEM, VMEM, VMEM],
        out_specs=[VMEM] * peers,
        scratch_shapes=[
            pltpu.VMEM((rows, features), jnp.float32),
            pltpu.VMEM((rows, wide), jnp.float32),
            pltpu.VMEM((peers, rows, wide), jnp.bfloat16),
        ],
        name="student",
        cost_estimate=cost(2 * rows * features * columns, 2 * features * columns),
    )(me, hidden, gain, projection)


def teacher_kernel(first_ref, second_ref, residual_ref, slots_ref, marks_ref, out_ref, late_ref, sems):
    rows, columns = residual_ref.shape
    half = columns // 2
    copies = [
        pltpu.make_async_copy(second_ref.at[k], late_ref.at[k], sems.at[k])
        for k in range(late_ref.shape[0])
    ]
    for copy in copies:
        copy.start()
    early = first_ref[0].astype(jnp.float32)
    for k in range(1, first_ref.shape[0]):
        early = early + first_ref[k].astype(jnp.float32)
    for copy in copies:
        copy.wait()
    late = late_ref[0].astype(jnp.float32)
    for k in range(1, late_ref.shape[0]):
        late = late + late_ref[k].astype(jnp.float32)
    summed = jnp.concatenate([early, late], axis=1)
    teacher = (residual_ref[...].astype(jnp.float32) + summed).astype(jnp.bfloat16)
    lines = lax.broadcasted_iota(jnp.int32, (out_ref.shape[0], rows), 0)
    full, low, high = (
        (lines == slots_ref[k : k + 1, :]).astype(jnp.float32).astype(jnp.bfloat16) for k in range(3)
    )

    def moved(select, part):
        return jnp.dot(select, part, preferred_element_type=jnp.float32)

    rest = moved(low, teacher[:, :half]) + moved(high, teacher[:, half:])
    out_ref[:, :columns] = moved(full, teacher).astype(jnp.bfloat16)
    out_ref[:, columns : columns + half] = rest.astype(jnp.bfloat16)
    out_ref[:, columns + half :] = moved(full + low + high, marks_ref[...]).astype(jnp.bfloat16)


def teacher_rows(first, second, residual, slots, marks, lines):
    rows, columns = residual.shape
    width = columns + columns // 2 + MARKS
    return pl.pallas_call(
        teacher_kernel,
        out_shape=jax.ShapeDtypeStruct((lines, width), jnp.bfloat16),
        in_specs=[VMEM, pl.BlockSpec(memory_space=pl.ANY)] + [VMEM] * 3,
        out_specs=VMEM,
        scratch_shapes=[
            pltpu.VMEM(second.shape, second.dtype),
            pltpu.SemaphoreType.DMA((second.shape[0],)),
        ],
        name="teacher_rows",
        cost_estimate=cost(2 * rows * width * lines, 16 * residual.size),
    )(first, second, residual, slots, marks)


def gradient_kernel(me_ref, rows_ref, *refs):
    student_refs, (sum_ref, max_ref) = refs[:-2], refs[-2:]
    height, columns = sum_ref.shape
    groups, per = len(student_refs), student_refs[0].shape[0]
    pred_at = lane_tiles(height)
    half = columns // 2
    lines, tokens = rows_ref.shape[0], groups * per
    marks = rows_ref[:, columns + half :].astype(jnp.float32).astype(jnp.int32)
    lanes = lax.broadcasted_iota(jnp.int32, (lines, tokens), 1)
    line = lax.broadcasted_iota(jnp.int32, (lines, tokens), 0)
    low_half = (line & (FULL - 1)) < REST

    def select(at, wanted):
        place = (marks[:, at : at + 1] ^ me_ref[0]) * per + marks[:, at + 1 : at + 2]
        return ((lanes == place) & wanted).astype(jnp.float32).astype(jnp.bfloat16)

    def placed(chosen, start):
        return lax.dot_general(
            chosen, rows_ref[:, start : start + half], ROWS_FIRST, preferred_element_type=jnp.float32
        )

    full = select(0, True)
    target = [
        placed(full, 0) + placed(select(2, low_half), columns),
        placed(full, half) + placed(select(2, ~low_half), columns),
    ]
    largest = jnp.zeros((1, 1), jnp.float32)
    for side in range(2):
        cols = slice(side * half, (side + 1) * half)
        total = None
        for g, ref in enumerate(student_refs):
            aimed = target[side][g * per : (g + 1) * per]
            pred = ref[:, pred_at + side * half : pred_at + (side + 1) * half]
            diff = (pred.astype(jnp.float32) - aimed).astype(jnp.bfloat16)
            part = lax.dot_general(
                ref[:, :height], diff, ROWS_FIRST, preferred_element_type=jnp.float32
            )
            largest = jnp.maximum(largest, jnp.max(jnp.abs(part), keepdims=True))
            total = part if total is None else total + part
        sum_ref[:, cols] = total.astype(jnp.bfloat16)
    max_ref[0, 0] = jnp.max(largest)


def gradient(me, rows, packed, height, columns):
    tokens = len(packed) * packed[0].shape[0]
    return pl.pallas_call(
        gradient_kernel,
        out_shape=(
            jax.ShapeDtypeStruct((height, columns), jnp.bfloat16),
            jax.ShapeDtypeStruct((1, 1), jnp.float32),
        ),
        in_specs=[SMEM, VMEM] + [VMEM] * len(packed),
        out_specs=(VMEM, SMEM),
        name="gradient",
        cost_estimate=cost(4 * tokens * height * columns, 4 * tokens * height),
    )(me, rows, *packed)


def per_device(student_hidden, norm_gain, projection, teacher_partials, teacher_residual, owner):
    rows_dev, columns = teacher_residual.shape
    features = student_hidden.shape[1]
    nx, nz, nc = (lax.axis_size(a) for a in (X, Z, C))
    peers = nx * nc
    block = features // (nx * nz * nc)
    assert rows_dev == nz * (FULL + REST)
    me = lax.axis_index(X) * nc + lax.axis_index(C)
    me_ref = me.reshape(1).astype(jnp.int32)

    partner = [(0, 1), (1, 0)]
    here = lax.axis_index(XH).reshape(1).astype(jnp.int32)
    own_terms = teacher_partials[0]
    direct = direct_columns(own_terms, lax.axis_size(TP))
    away = away_columns(1 - here, own_terms, lax.axis_size(Y))
    first = exchange(direct, TP)
    swapped = lax.ppermute(away, XH, partner)

    packed = student(me_ref, student_hidden, norm_gain[None], projection, (nx, nz, nc, block))
    packed = [packed[0]] + [to_peer(packed[k], k) for k in range(1, peers)]
    paired = pair_sum(here, own_terms, swapped)
    first, paired = lax.optimization_barrier((first, paired))
    second = exchange(paired, (Y,))

    whose = owner // rows_dev
    z_to = (whose // nc) % nz
    peer_to = (whose // (nz * nc)) * nc + whose % nc
    index = jnp.arange(rows_dev)
    earlier = (z_to[None, :] == z_to[:, None]) & (index[None, :] < index[:, None])
    rank = jnp.sum(earlier.astype(jnp.int32), axis=1)
    full = rank < FULL
    line = z_to * FULL + jnp.where(full, rank, rank - FULL)
    slots = jnp.stack([jnp.where(full, line, -1), jnp.where(full, -1, line)])
    slots = jnp.concatenate([slots, jnp.where(full, -1, line + REST)[None]])
    lane = lax.broadcasted_iota(jnp.int32, (rows_dev, MARKS), 1) - jnp.where(full, 0, 2)[:, None]
    marks = jnp.where(lane == 0, peer_to[:, None], (owner % rows_dev)[:, None])
    marks = jnp.where((lane == 0) | (lane == 1), marks, 0).astype(jnp.bfloat16)

    second, packed = lax.optimization_barrier((second, packed))

    outgoing = teacher_rows(first, second, teacher_residual, slots, marks, nz * FULL)
    arrived = exchange(outgoing.reshape(nz, FULL, -1), Z).reshape(nz * FULL, -1)
    rows = lax.all_gather(arrived, XC, axis=0, tiled=True)

    tile, largest = gradient(me_ref, rows, packed, nz * block, columns)
    pieces = exchange(tile.reshape(nz, block, columns), Z)
    scale = largest[0, 0]
    for axes in (C, (XH, X), Y, ZL, ZH):
        scale = lax.pmax(scale, axes)
    scale = scale + 1e-06
    return jnp.sum(pieces.astype(jnp.float32), axis=0) / scale


def solution(mesh):
    torus = Mesh(mesh.devices.reshape(2, 3, 4, 2, 2, 8), (X, ZH, ZL, C, XH, Y))
    placed = (P(DP, None), P(), P(None, TP), P(TP, DP, None), P(DP, TP), P(DP))
    return jax.shard_map(
        per_device, mesh=torus, in_specs=placed, out_specs=P(DP, TP), check_vma=False
    )
```

```python
import jax
import jax.numpy as jnp
from jax import lax
from jax.experimental import pallas as pl
from jax.experimental.pallas import tpu as pltpu
from jax.sharding import Mesh
from jax.sharding import PartitionSpec as P


X, ZH, ZL, C = "x_lo", "z_hi", "z_lo", "core"
XH, Y = "x_hi", "y"
DP, TP, XC, Z = (X, ZH, ZL, C), (XH, Y), (X, C), (ZH, ZL)
VMEM = pl.BlockSpec(memory_space=pltpu.VMEM)
SMEM = pl.BlockSpec(memory_space=pltpu.SMEM)
ROWS_FIRST = (((0,), (0,)), ((), ()))
MARKS, FULL, REST = 128, 8, 4


def exchange(array, axes):
    return lax.all_to_all(array, axes, split_axis=0, concat_axis=0, tiled=True)


def to_peer(array, k):
    return lax.ppermute(array, XC, [(p, p ^ k) for p in range(4)])


def cost(flops, moved):
    return pl.CostEstimate(flops=flops, bytes_accessed=moved, transcendentals=0)


def half_of(array):
    return pl.BlockSpec((array.shape[0], array.shape[1] // 2), lambda _, which: (0, which[0]))


def direct_kernel(in_ref, out_ref):
    parts, _, width = out_ref.shape
    for k in range(parts):
        out_ref[k] = in_ref[:, 2 * k * width : (2 * k + 1) * width]


def direct_columns(array, parts):
    rows, width = array.shape
    half = width // parts // 2
    return pl.pallas_call(
        direct_kernel,
        out_shape=jax.ShapeDtypeStruct((parts, rows, half), array.dtype),
        in_specs=[VMEM],
        out_specs=VMEM,
        name="direct_columns",
        cost_estimate=cost(0, 3 * array.size),
    )(array)


def away_kernel(_, in_ref, out_ref):
    parts, _, width = out_ref.shape
    for k in range(parts):
        out_ref[k] = in_ref[:, (2 * k + 1) * width : 2 * (k + 1) * width]


def away_columns(which, array, parts):
    rows, width = array.shape
    shape = (parts, rows, width // parts // 4)
    return pl.pallas_call(
        away_kernel,
        out_shape=jax.ShapeDtypeStruct(shape, array.dtype),
        grid_spec=pltpu.PrefetchScalarGridSpec(
            num_scalar_prefetch=1,
            grid=(1,),
            in_specs=[half_of(array)],
            out_specs=pl.BlockSpec(shape, lambda *_: (0, 0, 0)),
        ),
        name="away_columns",
        cost_estimate=cost(0, 2 * array.size),
    )(which, array)


def pair_kernel(_, in_ref, got_ref, out_ref):
    parts, _, width = got_ref.shape
    for k in range(parts):
        mine = in_ref[:, (2 * k + 1) * width : 2 * (k + 1) * width].astype(jnp.float32)
        out_ref[k] = (mine + got_ref[k].astype(jnp.float32)).astype(jnp.bfloat16)


def pair_sum(which, array, got):
    return pl.pallas_call(
        pair_kernel,
        out_shape=jax.ShapeDtypeStruct(got.shape, got.dtype),
        grid_spec=pltpu.PrefetchScalarGridSpec(
            num_scalar_prefetch=1,
            grid=(1,),
            in_specs=[half_of(array), pl.BlockSpec(got.shape, lambda *_: (0, 0, 0))],
            out_specs=pl.BlockSpec(got.shape, lambda *_: (0, 0, 0)),
        ),
        name="pair_sum",
        cost_estimate=cost(got.size, 6 * got.size),
    )(which, array, got)


def lane_tiles(width):
    return -(-width // 128) * 128


def student_kernel(sizes, me_ref, hidden_ref, gain_ref, proj_ref, *refs):
    nx, nz, nc, block = sizes
    peers = nx * nc
    out_refs, (wide_ref, line_ref, parts_ref) = refs[:peers], refs[peers:]
    values = hidden_ref[...].astype(jnp.float32)
    inverse = lax.rsqrt(jnp.mean(values * values, axis=-1, keepdims=True) + 1e-05)
    normed = values * inverse * gain_ref[...]
    pred = jnp.dot(normed.astype(jnp.bfloat16), proj_ref[...], preferred_element_type=jnp.float32)
    pred = pred.astype(jnp.bfloat16)
    wide_ref[...] = normed
    line_ref[...] = jnp.zeros_like(line_ref)
    for p in range(peers):
        x, c = p // nc, p % nc
        for z in range(nz):
            start = ((x * nz + z) * nc + c) * block
            line_ref[:, z * block : (z + 1) * block] = wide_ref[:, start : start + block]
        parts_ref[p] = line_ref[...].astype(jnp.bfloat16)
    at = line_ref.shape[-1]
    for k in range(peers):
        out_refs[k][:, :at] = parts_ref[me_ref[0] ^ k]
        out_refs[k][:, at:] = pred


def student(me, hidden, gain, projection, sizes):
    nx, nz, nc, block = sizes
    rows, features = hidden.shape
    columns = projection.shape[1]
    peers, wide = nx * nc, lane_tiles(nz * block)
    return pl.pallas_call(
        lambda *refs: student_kernel(sizes, *refs),
        out_shape=[jax.ShapeDtypeStruct((rows, wide + columns), jnp.bfloat16)] * peers,
        in_specs=[SMEM, VMEM, VMEM, VMEM],
        out_specs=[VMEM] * peers,
        scratch_shapes=[
            pltpu.VMEM((rows, features), jnp.float32),
            pltpu.VMEM((rows, wide), jnp.float32),
            pltpu.VMEM((peers, rows, wide), jnp.bfloat16),
        ],
        name="student",
        cost_estimate=cost(2 * rows * features * columns, 2 * features * columns),
    )(me, hidden, gain, projection)


def teacher_kernel(first_ref, second_ref, residual_ref, slots_ref, marks_ref, out_ref, late_ref, sems):
    rows, columns = residual_ref.shape
    half = columns // 2
    copies = [
        pltpu.make_async_copy(second_ref.at[k], late_ref.at[k], sems.at[k])
        for k in range(late_ref.shape[0])
    ]
    for copy in copies:
        copy.start()
    early = first_ref[0].astype(jnp.float32)
    for k in range(1, first_ref.shape[0]):
        early = early + first_ref[k].astype(jnp.float32)
    for copy in copies:
        copy.wait()
    late = late_ref[0].astype(jnp.float32)
    for k in range(1, late_ref.shape[0]):
        late = late + late_ref[k].astype(jnp.float32)
    summed = jnp.concatenate([early, late], axis=1)
    teacher = (residual_ref[...].astype(jnp.float32) + summed).astype(jnp.bfloat16)
    lines = lax.broadcasted_iota(jnp.int32, (out_ref.shape[0], rows), 0)
    full, low, high = (
        (lines == slots_ref[k : k + 1, :]).astype(jnp.float32).astype(jnp.bfloat16) for k in range(3)
    )

    def moved(select, part):
        return jnp.dot(select, part, preferred_element_type=jnp.float32)

    rest = moved(low, teacher[:, :half]) + moved(high, teacher[:, half:])
    out_ref[:, :columns] = moved(full, teacher).astype(jnp.bfloat16)
    out_ref[:, columns : columns + half] = rest.astype(jnp.bfloat16)
    out_ref[:, columns + half :] = moved(full + low + high, marks_ref[...]).astype(jnp.bfloat16)


def teacher_rows(first, second, residual, slots, marks, lines):
    rows, columns = residual.shape
    width = columns + columns // 2 + MARKS
    return pl.pallas_call(
        teacher_kernel,
        out_shape=jax.ShapeDtypeStruct((lines, width), jnp.bfloat16),
        in_specs=[VMEM, pl.BlockSpec(memory_space=pl.ANY)] + [VMEM] * 3,
        out_specs=VMEM,
        scratch_shapes=[
            pltpu.VMEM(second.shape, second.dtype),
            pltpu.SemaphoreType.DMA((second.shape[0],)),
        ],
        name="teacher_rows",
        cost_estimate=cost(2 * rows * width * lines, 16 * residual.size),
    )(first, second, residual, slots, marks)


def gradient_kernel(me_ref, rows_ref, *refs):
    student_refs, (sum_ref, max_ref) = refs[:-2], refs[-2:]
    height, columns = sum_ref.shape
    groups, per = len(student_refs), student_refs[0].shape[0]
    pred_at = lane_tiles(height)
    half = columns // 2
    lines, tokens = rows_ref.shape[0], groups * per
    marks = rows_ref[:, columns + half :].astype(jnp.float32).astype(jnp.int32)
    lanes = lax.broadcasted_iota(jnp.int32, (lines, tokens), 1)
    line = lax.broadcasted_iota(jnp.int32, (lines, tokens), 0)
    low_half = (line & (FULL - 1)) < REST

    def select(at, wanted):
        place = (marks[:, at : at + 1] ^ me_ref[0]) * per + marks[:, at + 1 : at + 2]
        return ((lanes == place) & wanted).astype(jnp.float32).astype(jnp.bfloat16)

    def placed(chosen, start):
        return lax.dot_general(
            chosen, rows_ref[:, start : start + half], ROWS_FIRST, preferred_element_type=jnp.float32
        )

    full = select(0, True)
    target = [
        placed(full, 0) + placed(select(2, low_half), columns),
        placed(full, half) + placed(select(2, ~low_half), columns),
    ]
    largest = jnp.zeros((1, 1), jnp.float32)
    for side in range(2):
        cols = slice(side * half, (side + 1) * half)
        total = None
        for g, ref in enumerate(student_refs):
            aimed = target[side][g * per : (g + 1) * per]
            pred = ref[:, pred_at + side * half : pred_at + (side + 1) * half]
            diff = (pred.astype(jnp.float32) - aimed).astype(jnp.bfloat16)
            part = lax.dot_general(
                ref[:, :height], diff, ROWS_FIRST, preferred_element_type=jnp.float32
            )
            largest = jnp.maximum(largest, jnp.max(jnp.abs(part), keepdims=True))
            total = part if total is None else total + part
        sum_ref[:, cols] = total.astype(jnp.bfloat16)
    max_ref[0, 0] = jnp.max(largest)


def gradient(me, rows, packed, height, columns):
    tokens = len(packed) * packed[0].shape[0]
    return pl.pallas_call(
        gradient_kernel,
        out_shape=(
            jax.ShapeDtypeStruct((height, columns), jnp.bfloat16),
            jax.ShapeDtypeStruct((1, 1), jnp.float32),
        ),
        in_specs=[SMEM, VMEM] + [VMEM] * len(packed),
        out_specs=(VMEM, SMEM),
        name="gradient",
        cost_estimate=cost(4 * tokens * height * columns, 4 * tokens * height),
    )(me, rows, *packed)


def per_device(student_hidden, norm_gain, projection, teacher_partials, teacher_residual, owner):
    rows_dev, columns = teacher_residual.shape
    features = student_hidden.shape[1]
    nx, nz, nc = (lax.axis_size(a) for a in (X, Z, C))
    peers = nx * nc
    block = features // (nx * nz * nc)
    assert rows_dev == nz * (FULL + REST)
    me = lax.axis_index(X) * nc + lax.axis_index(C)
    me_ref = me.reshape(1).astype(jnp.int32)

    partner = [(0, 1), (1, 0)]
    here = lax.axis_index(XH).reshape(1).astype(jnp.int32)
    own_terms = teacher_partials[0]
    direct = direct_columns(own_terms, lax.axis_size(TP))
    away = away_columns(1 - here, own_terms, lax.axis_size(Y))
    first = exchange(direct, TP)
    swapped = lax.ppermute(away, XH, partner)

    packed = student(me_ref, student_hidden, norm_gain[None], projection, (nx, nz, nc, block))
    near = [to_peer(packed[k], k) for k in range(1, nc)]
    far = [to_peer(packed[k], k) for k in range(nc, peers)]
    packed = [packed[0]] + near + far
    paired = pair_sum(here, own_terms, swapped)
    first, paired = lax.optimization_barrier((first, paired))
    second = exchange(paired, (Y,))

    whose = owner // rows_dev
    z_to = (whose // nc) % nz
    peer_to = (whose // (nz * nc)) * nc + whose % nc
    index = jnp.arange(rows_dev)
    earlier = (z_to[None, :] == z_to[:, None]) & (index[None, :] < index[:, None])
    rank = jnp.sum(earlier.astype(jnp.int32), axis=1)
    full = rank < FULL
    line = z_to * FULL + jnp.where(full, rank, rank - FULL)
    slots = jnp.stack([jnp.where(full, line, -1), jnp.where(full, -1, line)])
    slots = jnp.concatenate([slots, jnp.where(full, -1, line + REST)[None]])
    lane = lax.broadcasted_iota(jnp.int32, (rows_dev, MARKS), 1) - jnp.where(full, 0, 2)[:, None]
    marks = jnp.where(lane == 0, peer_to[:, None], (owner % rows_dev)[:, None])
    marks = jnp.where((lane == 0) | (lane == 1), marks, 0).astype(jnp.bfloat16)

    second, packed = lax.optimization_barrier((second, packed))

    outgoing = teacher_rows(first, second, teacher_residual, slots, marks, nz * FULL)
    arrived = exchange(outgoing.reshape(nz, FULL, -1), Z).reshape(nz * FULL, -1)
    rows = lax.all_gather(arrived, X, axis=0, tiled=True)
    rows = lax.all_gather(rows, C, axis=0, tiled=True)

    tile, largest = gradient(me_ref, rows, packed, nz * block, columns)
    pieces = exchange(tile.reshape(nz, block, columns), Z)
    scale = largest[0, 0]
    for axes in (C, (XH, X), Y, ZL, ZH):
        scale = lax.pmax(scale, axes)
    scale = scale + 1e-06
    return jnp.sum(pieces.astype(jnp.float32), axis=0) / scale


def solution(mesh):
    torus = Mesh(mesh.devices.reshape(2, 3, 4, 2, 2, 8), (X, ZH, ZL, C, XH, Y))
    placed = (P(DP, None), P(), P(None, TP), P(TP, DP, None), P(DP, TP), P(DP))
    return jax.shard_map(
        per_device, mesh=torus, in_specs=placed, out_specs=P(DP, TP), check_vma=False
    )
```

```python
import jax
import jax.numpy as jnp
from jax import lax
from jax.experimental import pallas as pl
from jax.experimental.pallas import tpu as pltpu
from jax.sharding import Mesh
from jax.sharding import PartitionSpec as P


X, ZH, ZL, C = "x_lo", "z_hi", "z_lo", "core"
XH, Y = "x_hi", "y"
DP, TP, XC, Z = (X, ZH, ZL, C), (XH, Y), (X, C), (ZH, ZL)
VMEM = pl.BlockSpec(memory_space=pltpu.VMEM)
SMEM = pl.BlockSpec(memory_space=pltpu.SMEM)
ROWS_FIRST = (((0,), (0,)), ((), ()))
MARKS, FULL, REST = 128, 8, 4


def exchange(array, axes):
    return lax.all_to_all(array, axes, split_axis=0, concat_axis=0, tiled=True)


def to_peer(array, k):
    return lax.ppermute(array, XC, [(p, p ^ k) for p in range(4)])


def cost(flops, moved):
    return pl.CostEstimate(flops=flops, bytes_accessed=moved, transcendentals=0)


def half_of(array):
    return pl.BlockSpec((array.shape[0], array.shape[1] // 2), lambda _, which: (0, which[0]))


def direct_kernel(in_ref, out_ref):
    parts, _, width = out_ref.shape
    half = width // 2
    for side in range(2):
        for k in range(parts):
            start = (side * parts + k) * width
            out_ref[k, :, side * half : (side + 1) * half] = in_ref[:, start : start + half]


def direct_columns(array, parts):
    rows, width = array.shape
    return pl.pallas_call(
        direct_kernel,
        out_shape=jax.ShapeDtypeStruct((parts, rows, width // parts // 2), array.dtype),
        in_specs=[VMEM],
        out_specs=VMEM,
        name="direct_columns",
        cost_estimate=cost(0, 3 * array.size),
    )(array)


def half_sum_kernel(here_ref, terms_ref, keep_ref, send_ref, total_ref):
    total = terms_ref[0].astype(jnp.float32)
    for k in range(1, terms_ref.shape[0]):
        total = total + terms_ref[k].astype(jnp.float32)
    total_ref[...] = total
    half = keep_ref.shape[-1]
    mine = pl.multiple_of(here_ref[0] * half, half)
    other = pl.multiple_of((1 - here_ref[0]) * half, half)
    keep_ref[...] = total_ref[:, pl.ds(mine, half)]
    send_ref[...] = total_ref[:, pl.ds(other, half)].astype(jnp.bfloat16)


def half_sum(here, terms):
    _, rows, width = terms.shape
    shape = (rows, width // 2)
    return pl.pallas_call(
        half_sum_kernel,
        out_shape=(
            jax.ShapeDtypeStruct(shape, jnp.float32),
            jax.ShapeDtypeStruct(shape, jnp.bfloat16),
        ),
        in_specs=[SMEM, VMEM],
        out_specs=(VMEM, VMEM),
        scratch_shapes=[pltpu.VMEM((rows, width), jnp.float32)],
        name="half_sum",
        cost_estimate=cost(terms.size, 2 * terms.size),
    )(here, terms)


def away_kernel(_, in_ref, out_ref):
    parts, _, width = out_ref.shape
    for k in range(parts):
        out_ref[k] = in_ref[:, (2 * k + 1) * width : 2 * (k + 1) * width]


def away_columns(which, array, parts):
    rows, width = array.shape
    shape = (parts, rows, width // parts // 4)
    return pl.pallas_call(
        away_kernel,
        out_shape=jax.ShapeDtypeStruct(shape, array.dtype),
        grid_spec=pltpu.PrefetchScalarGridSpec(
            num_scalar_prefetch=1,
            grid=(1,),
            in_specs=[half_of(array)],
            out_specs=pl.BlockSpec(shape, lambda *_: (0, 0, 0)),
        ),
        name="away_columns",
        cost_estimate=cost(0, 2 * array.size),
    )(which, array)


def pair_kernel(_, in_ref, got_ref, out_ref):
    parts, _, width = got_ref.shape
    for k in range(parts):
        mine = in_ref[:, (2 * k + 1) * width : 2 * (k + 1) * width].astype(jnp.float32)
        out_ref[k] = (mine + got_ref[k].astype(jnp.float32)).astype(jnp.bfloat16)


def pair_sum(which, array, got):
    return pl.pallas_call(
        pair_kernel,
        out_shape=jax.ShapeDtypeStruct(got.shape, got.dtype),
        grid_spec=pltpu.PrefetchScalarGridSpec(
            num_scalar_prefetch=1,
            grid=(1,),
            in_specs=[half_of(array), pl.BlockSpec(got.shape, lambda *_: (0, 0, 0))],
            out_specs=pl.BlockSpec(got.shape, lambda *_: (0, 0, 0)),
        ),
        name="pair_sum",
        cost_estimate=cost(got.size, 6 * got.size),
    )(which, array, got)


def lane_tiles(width):
    return -(-width // 128) * 128


def student_kernel(sizes, me_ref, hidden_ref, gain_ref, proj_ref, *refs):
    nx, nz, nc, block = sizes
    peers = nx * nc
    out_refs, (wide_ref, line_ref, parts_ref) = refs[:peers], refs[peers:]
    values = hidden_ref[...].astype(jnp.float32)
    inverse = lax.rsqrt(jnp.mean(values * values, axis=-1, keepdims=True) + 1e-05)
    normed = values * inverse * gain_ref[...]
    pred = jnp.dot(normed.astype(jnp.bfloat16), proj_ref[...], preferred_element_type=jnp.float32)
    pred = pred.astype(jnp.bfloat16)
    wide_ref[...] = normed
    line_ref[...] = jnp.zeros_like(line_ref)
    for p in range(peers):
        x, c = p // nc, p % nc
        for z in range(nz):
            start = ((x * nz + z) * nc + c) * block
            line_ref[:, z * block : (z + 1) * block] = wide_ref[:, start : start + block]
        parts_ref[p] = line_ref[...].astype(jnp.bfloat16)
    at = line_ref.shape[-1]
    for k in range(peers):
        out_refs[k][:, :at] = parts_ref[me_ref[0] ^ k]
        out_refs[k][:, at:] = pred


def student(me, hidden, gain, projection, sizes):
    nx, nz, nc, block = sizes
    rows, features = hidden.shape
    columns = projection.shape[1]
    peers, wide = nx * nc, lane_tiles(nz * block)
    return pl.pallas_call(
        lambda *refs: student_kernel(sizes, *refs),
        out_shape=[jax.ShapeDtypeStruct((rows, wide + columns), jnp.bfloat16)] * peers,
        in_specs=[SMEM, VMEM, VMEM, VMEM],
        out_specs=[VMEM] * peers,
        scratch_shapes=[
            pltpu.VMEM((rows, features), jnp.float32),
            pltpu.VMEM((rows, wide), jnp.float32),
            pltpu.VMEM((peers, rows, wide), jnp.bfloat16),
        ],
        name="student",
        cost_estimate=cost(2 * rows * features * columns, 2 * features * columns),
    )(me, hidden, gain, projection)


def teacher_kernel(keep_ref, got_ref, second_ref, residual_ref, slots_ref, marks_ref, out_ref, late_ref, sems):
    rows, columns = residual_ref.shape
    half = columns // 2
    copies = [
        pltpu.make_async_copy(second_ref.at[k], late_ref.at[k], sems.at[k])
        for k in range(late_ref.shape[0])
    ]
    for copy in copies:
        copy.start()
    early = keep_ref[...] + got_ref[...].astype(jnp.float32)
    for copy in copies:
        copy.wait()
    late = late_ref[0].astype(jnp.float32)
    for k in range(1, late_ref.shape[0]):
        late = late + late_ref[k].astype(jnp.float32)
    summed = jnp.concatenate([early, late], axis=1)
    teacher = (residual_ref[...].astype(jnp.float32) + summed).astype(jnp.bfloat16)
    lines = lax.broadcasted_iota(jnp.int32, (out_ref.shape[0], rows), 0)
    full, low, high = (
        (lines == slots_ref[k : k + 1, :]).astype(jnp.float32).astype(jnp.bfloat16) for k in range(3)
    )

    def moved(select, part):
        return jnp.dot(select, part, preferred_element_type=jnp.float32)

    rest = moved(low, teacher[:, :half]) + moved(high, teacher[:, half:])
    out_ref[:, :columns] = moved(full, teacher).astype(jnp.bfloat16)
    out_ref[:, columns : columns + half] = rest.astype(jnp.bfloat16)
    out_ref[:, columns + half :] = moved(full + low + high, marks_ref[...]).astype(jnp.bfloat16)


def teacher_rows(keep, got, second, residual, slots, marks, lines):
    rows, columns = residual.shape
    width = columns + columns // 2 + MARKS
    return pl.pallas_call(
        teacher_kernel,
        out_shape=jax.ShapeDtypeStruct((lines, width), jnp.bfloat16),
        in_specs=[VMEM, VMEM, pl.BlockSpec(memory_space=pl.ANY)] + [VMEM] * 3,
        out_specs=VMEM,
        scratch_shapes=[
            pltpu.VMEM(second.shape, second.dtype),
            pltpu.SemaphoreType.DMA((second.shape[0],)),
        ],
        name="teacher_rows",
        cost_estimate=cost(2 * rows * width * lines, 16 * residual.size),
    )(keep, got, second, residual, slots, marks)


def gradient_kernel(me_ref, rows_ref, *refs):
    student_refs, (sum_ref, max_ref) = refs[:-2], refs[-2:]
    height, columns = sum_ref.shape
    groups, per = len(student_refs), student_refs[0].shape[0]
    pred_at = lane_tiles(height)
    half = columns // 2
    lines, tokens = rows_ref.shape[0], groups * per
    marks = rows_ref[:, columns + half :].astype(jnp.float32).astype(jnp.int32)
    lanes = lax.broadcasted_iota(jnp.int32, (lines, tokens), 1)
    line = lax.broadcasted_iota(jnp.int32, (lines, tokens), 0)
    low_half = (line & (FULL - 1)) < REST

    def select(at, wanted):
        place = (marks[:, at : at + 1] ^ me_ref[0]) * per + marks[:, at + 1 : at + 2]
        return ((lanes == place) & wanted).astype(jnp.float32).astype(jnp.bfloat16)

    def placed(chosen, start):
        return lax.dot_general(
            chosen, rows_ref[:, start : start + half], ROWS_FIRST, preferred_element_type=jnp.float32
        )

    full = select(0, True)
    target = [
        placed(full, 0) + placed(select(2, low_half), columns),
        placed(full, half) + placed(select(2, ~low_half), columns),
    ]
    largest = jnp.zeros((1, 1), jnp.float32)
    for side in range(2):
        cols = slice(side * half, (side + 1) * half)
        total = None
        for g, ref in enumerate(student_refs):
            aimed = target[side][g * per : (g + 1) * per]
            pred = ref[:, pred_at + side * half : pred_at + (side + 1) * half]
            diff = (pred.astype(jnp.float32) - aimed).astype(jnp.bfloat16)
            part = lax.dot_general(
                ref[:, :height], diff, ROWS_FIRST, preferred_element_type=jnp.float32
            )
            largest = jnp.maximum(largest, jnp.max(jnp.abs(part), keepdims=True))
            total = part if total is None else total + part
        sum_ref[:, cols] = total.astype(jnp.bfloat16)
    max_ref[0, 0] = jnp.max(largest)


def gradient(me, rows, packed, height, columns):
    tokens = len(packed) * packed[0].shape[0]
    return pl.pallas_call(
        gradient_kernel,
        out_shape=(
            jax.ShapeDtypeStruct((height, columns), jnp.bfloat16),
            jax.ShapeDtypeStruct((1, 1), jnp.float32),
        ),
        in_specs=[SMEM, VMEM] + [VMEM] * len(packed),
        out_specs=(VMEM, SMEM),
        name="gradient",
        cost_estimate=cost(4 * tokens * height * columns, 4 * tokens * height),
    )(me, rows, *packed)


def per_device(student_hidden, norm_gain, projection, teacher_partials, teacher_residual, owner):
    rows_dev, columns = teacher_residual.shape
    features = student_hidden.shape[1]
    nx, nz, nc = (lax.axis_size(a) for a in (X, Z, C))
    peers = nx * nc
    block = features // (nx * nz * nc)
    assert rows_dev == nz * (FULL + REST)
    me = lax.axis_index(X) * nc + lax.axis_index(C)
    me_ref = me.reshape(1).astype(jnp.int32)

    partner = [(0, 1), (1, 0)]
    here = lax.axis_index(XH).reshape(1).astype(jnp.int32)
    own_terms = teacher_partials[0]
    direct = direct_columns(own_terms, lax.axis_size(Y))
    away = away_columns(1 - here, own_terms, lax.axis_size(Y))
    first = exchange(direct, (Y,))
    swapped = lax.ppermute(away, XH, partner)

    packed = student(me_ref, student_hidden, norm_gain[None], projection, (nx, nz, nc, block))
    packed = [packed[0]] + [to_peer(packed[k], k) for k in range(1, peers)]
    paired = pair_sum(here, own_terms, swapped)
    first, paired = lax.optimization_barrier((first, paired))
    second = exchange(paired, (Y,))
    keep, send = half_sum(here, first)
    got = lax.ppermute(send, XH, partner)

    whose = owner // rows_dev
    z_to = (whose // nc) % nz
    peer_to = (whose // (nz * nc)) * nc + whose % nc
    index = jnp.arange(rows_dev)
    earlier = (z_to[None, :] == z_to[:, None]) & (index[None, :] < index[:, None])
    rank = jnp.sum(earlier.astype(jnp.int32), axis=1)
    full = rank < FULL
    line = z_to * FULL + jnp.where(full, rank, rank - FULL)
    slots = jnp.stack([jnp.where(full, line, -1), jnp.where(full, -1, line)])
    slots = jnp.concatenate([slots, jnp.where(full, -1, line + REST)[None]])
    lane = lax.broadcasted_iota(jnp.int32, (rows_dev, MARKS), 1) - jnp.where(full, 0, 2)[:, None]
    marks = jnp.where(lane == 0, peer_to[:, None], (owner % rows_dev)[:, None])
    marks = jnp.where((lane == 0) | (lane == 1), marks, 0).astype(jnp.bfloat16)

    second, packed, got = lax.optimization_barrier((second, packed, got))

    outgoing = teacher_rows(keep, got, second, teacher_residual, slots, marks, nz * FULL)
    arrived = exchange(outgoing.reshape(nz, FULL, -1), Z).reshape(nz * FULL, -1)
    rows = lax.all_gather(arrived, XC, axis=0, tiled=True)

    tile, largest = gradient(me_ref, rows, packed, nz * block, columns)
    pieces = exchange(tile.reshape(nz, block, columns), Z)
    scale = largest[0, 0]
    for axes in (C, (XH, X), Y, ZL, ZH):
        scale = lax.pmax(scale, axes)
    scale = scale + 1e-06
    return jnp.sum(pieces.astype(jnp.float32), axis=0) / scale


def solution(mesh):
    torus = Mesh(mesh.devices.reshape(2, 3, 4, 2, 2, 8), (X, ZH, ZL, C, XH, Y))
    placed = (P(DP, None), P(), P(None, TP), P(TP, DP, None), P(DP, TP), P(DP))
    return jax.shard_map(
        per_device, mesh=torus, in_specs=placed, out_specs=P(DP, TP), check_vma=False
    )
```
